32 devices in a mesh: py: 8 (over y, x, core), px: 4 (over z).
Axes of the slice: x: 2, y: 2, z: 4, core: 2. Of those that a mesh axis runs over, the one named last changes fastest.
Arguments:
- source_terms: float32 [512, 512, 256], P('py', 'px'), may hold values from -6 to 6
- initial_values: float32 [512, 512, 256], P('py', 'px'), may hold values from -6 to 6
- absorption: float32 [512, 512, 256], P('py', 'px'), may hold values from 0.1 to 0.9
Outputs:
- improved: float32 [512, 512, 256], P('py', 'px')
The draws below stay inside these ranges and needn't reach their ends.
All inputs are finite; a program needn't handle non-finite values.
Results may differ from the reference program's by a relative error of at most 0.00002.
Values sent between devices are 32-bit elements; how exact they have to be, the bound alone decides.
A program may use at most 128 MiB of HBM per device.

```python
import jax
import jax.numpy as jnp
from jax import lax

CASES = 256
RATIO = 4
BEFORE = 2
AFTER = 2
INNER = 13
GRID_Y = 512
GRID_X = 512


def block_scale(rng, extent, pieces, low, largest):
    level = 1.0
    for position, shards_of in pieces:
        steps = jax.random.uniform(jax.random.fold_in(jax.random.fold_in(rng, 6), position), (shards_of,), jnp.float32, low / len(pieces), largest / len(pieces))
        level = level * jnp.repeat(jnp.exp(steps), extent[position] // shards_of).reshape((-1,) + (1,) * (len(extent) - 1 - position))
    return level


def noise(key, dims, scale, limit, split=(), dtype=jnp.bfloat16):
    loudness = block_scale(key, dims, split, -0.22, 0.18) if split else 1.0
    drawn = jax.random.normal(key, dims, jnp.float32) * scale * loudness
    return jnp.minimum(jnp.maximum(drawn, -limit), limit).astype(dtype)


def setup_inputs(seed: int = 0) -> dict:
    keys = jax.random.split(jax.random.key(seed), 4)
    return {
        "source_terms": noise(keys[0], (GRID_Y, GRID_X, CASES), 1.0, 6.0, ((0, 8), (1, 4)), jnp.float32),
        "initial_values": noise(keys[1], (GRID_Y, GRID_X, CASES), 1.0, 6.0, ((0, 8), (1, 4)), jnp.float32),
        "absorption": jnp.clip(0.1 + 0.79999997 * jax.random.uniform(keys[2], (GRID_Y, GRID_X, CASES), jnp.float32) ** block_scale(keys[2], (GRID_Y, GRID_X, CASES), ((0, 8), (1, 4)), -0.2, 0.2), 0.1, 0.9),
    }


def around_sum(padded):
    inner_y, inner_x = padded.shape[0] - 2, padded.shape[1] - 2
    middle_rows = lax.slice_in_dim(padded, 1, 1 + inner_y, axis=0)
    middle_columns = lax.slice_in_dim(padded, 1, 1 + inner_x, axis=1)
    return (lax.slice_in_dim(middle_columns, 0, inner_y, axis=0) + lax.slice_in_dim(middle_columns, 2, 2 + inner_y, axis=0)
            + lax.slice_in_dim(middle_rows, 0, inner_x, axis=1) + lax.slice_in_dim(middle_rows, 2, 2 + inner_x, axis=1))


def relax_once(padded, values, load, mass_here):
    return values + 0.8 * (load + around_sum(padded) - (4.0 + mass_here) * values) / (4.0 + mass_here)


def block_means(values):
    cut = values.reshape(values.shape[0] // RATIO, RATIO, values.shape[1] // RATIO, RATIO, values.shape[2])
    return jnp.mean(cut, axis=(1, 3))


def spread_blocks(values):
    return jnp.repeat(jnp.repeat(values, RATIO, axis=0), RATIO, axis=1)


def reference(source_terms, initial_values, absorption):
    values = initial_values
    for sweep in range(BEFORE):
        values = relax_once(jnp.pad(values, ((1, 1), (1, 1), (0, 0)), mode="wrap"), values, source_terms, absorption)
    defect = source_terms + around_sum(jnp.pad(values, ((1, 1), (1, 1), (0, 0)), mode="wrap")) - (4.0 + absorption) * values
    coarse_load, coarse_mass = block_means(defect) * RATIO, block_means(absorption) * RATIO
    coarse_values = jnp.zeros_like(coarse_load)
    for sweep in range(INNER):
        coarse_values = relax_once(jnp.pad(coarse_values, ((1, 1), (1, 1), (0, 0)), mode="wrap"), coarse_values, coarse_load, coarse_mass)
    values = values + spread_blocks(coarse_values)
    for sweep in range(AFTER):
        values = relax_once(jnp.pad(values, ((1, 1), (1, 1), (0, 0)), mode="wrap"), values, source_terms, absorption)
    improved = values
    return improved
```

```python
import functools

import jax
import jax.numpy as jnp
from jax import lax
from jax.experimental import pallas as pl
from jax.experimental.pallas import tpu as pltpu
from jax.sharding import PartitionSpec as P

RATIO = 4
INNER = 13
LANES = 128
DEEP = 7
MESH = pl.DeviceIdType.MESH
CHUNKS = 4


def kernel(shape, s_hbm, u_hbm, a_hbm, out_hbm, U, V, S, Q, R, D, CL, CR, CA, CB, CE, SP,
           RR, RC, PC, in_sem, out_sem, fs_sem, fr_sem, cs_sem, cr_sem):
    H, W, halves = shape
    HC, WC = H // RATIO, W // RATIO
    XW = W + 16
    npy, npx = lax.axis_size("py"), lax.axis_size("px")
    py, px = lax.axis_index("py"), lax.axis_index("px")
    ypos = {-1: lax.rem(py + npy - 1, npy), 0: py, 1: lax.rem(py + 1, npy)}
    xpos = {-1: lax.rem(px + npx - 1, npx), 0: px, 1: lax.rem(px + 1, npx)}
    eight = [(dy, dx) for dy in (-1, 0, 1) for dx in (-1, 0, 1) if dy or dx]

    def load(hbm, dst, row0, rows, half, sem):
        return pltpu.make_async_copy(
            hbm.at[pl.ds(row0, rows), :, pl.ds(half * LANES, LANES)], dst, sem)

    u_loads = [load(u_hbm, U.at[h, pl.ds(1, H), pl.ds(8, W), :], 0, H, h, in_sem.at[0, 0, h])
               for h in range(halves)]
    for c in u_loads:
        c.start()
    step = H // CHUNKS
    chunk_loads = []
    for k in range(CHUNKS):
        row = []
        for h in range(halves):
            row.append(load(a_hbm, Q.at[h, pl.ds(k * step, step)], k * step, step, h,
                            in_sem.at[1, k, h]))
        for c in row:
            c.start()
        chunk_loads.append(row)
    s_loads = [load(s_hbm, S.at[h], 0, H, h, in_sem.at[2, 0, h]) for h in range(halves)]
    for c in s_loads:
        c.start()

    barrier = pltpu.get_barrier_semaphore()
    for dy, dx in eight:
        pl.semaphore_signal(barrier, inc=1, device_id={"py": ypos[dy], "px": xpos[dx]},
                            device_id_type=MESH)
    pl.semaphore_wait(barrier, 8)

    def flat(buf):
        return buf.reshape(halves * (H + 2) * XW, LANES)

    def send_fine(buf, k):
        rows = []
        for n, (dy, row) in enumerate(((-1, 1), (1, H))):
            c = pltpu.make_async_remote_copy(
                src_ref=buf.at[:, row, pl.ds(8, W), :], dst_ref=RR.at[k, n],
                send_sem=fs_sem.at[k, n], recv_sem=fr_sem.at[k, n],
                device_id={"py": ypos[dy], "px": px}, device_id_type=MESH)
            c.start()
            rows.append(c)
        f = flat(buf)
        for n, (dx, col) in enumerate(((-1, 8), (1, 7 + W))):
            for h in range(halves):
                for g in range(0, H, 8):
                    PC[k, n, h, g:g + 8, :] = f[
                        pl.ds((h * (H + 2) + 1 + g) * XW + col, 8, stride=XW), :]
            c = pltpu.make_async_remote_copy(
                src_ref=PC.at[k, n], dst_ref=RC.at[k, n],
                send_sem=fs_sem.at[k, 2 + n], recv_sem=fr_sem.at[k, 2 + n],
                device_id={"py": py, "px": xpos[dx]}, device_id_type=MESH)
            c.start()
            rows.append(c)
        return rows

    def land_fine(buf, k, copies):
        for c in copies:
            c.wait()
        for n, row in enumerate((H + 1, 0)):
            for h in range(halves):
                buf[h, row, 8:8 + W, :] = RR[k, n, h]
        f = flat(buf)
        for n, col in enumerate((8 + W, 7)):
            for h in range(halves):
                for g in range(0, H, 8):
                    f[pl.ds((h * (H + 2) + 1 + g) * XW + col, 8, stride=XW), :] = (
                        RC[k, n, h, g:g + 8, :])

    def around(buf, h, Y, x):
        base = RATIO * Y
        c = [buf[h, base + i, x:x + 8, :] for i in range(RATIO + 2)]
        for i in range(RATIO):
            left = buf[h, base + 1 + i, x - 1:x + 7, :]
            right = buf[h, base + 1 + i, x + 1:x + 9, :]
            yield base + i, c[i + 1], (c[i] + c[i + 2]) + (left + right)

    def relax(src, dst):
        def unit(h, Y, x):
            for y, mid, nb in around(src, h, Y, x):
                dst[h, y + 1, x:x + 8, :] = (
                    0.2 * mid + (S[h, y, x - 8:x, :] + nb) * R[h, y, x - 8:x, :])
        return unit

    def defect(src):
        def unit(h, Y, x):
            total = None
            for y, mid, nb in around(src, h, Y, x):
                d = (S[h, y, x - 8:x, :] + nb) - Q[h, y, x - 8:x, :] * mid
                total = d if total is None else total + d
            D[h, Y, x - 8:x, :] = total
        return unit

    def inner(unit):
        @pl.loop(0, halves * (HC - 2))
        def _(i):
            h, Y = i // (HC - 2), 1 + i % (HC - 2)
            for x in range(16, W, 8):
                unit(h, Y, x)

    def rim(unit):
        @pl.loop(0, halves * 2)
        def _(i):
            h, Y = i // 2, (i % 2) * (HC - 1)
            for x in range(8, W + 8, 8):
                unit(h, Y, x)

        @pl.loop(0, halves * (HC - 2))
        def _(i):
            h, Y = i // (HC - 2), 1 + i % (HC - 2)
            unit(h, Y, 8)
            unit(h, Y, W)

    def reduce_into(dst, f):
        @pl.loop(0, halves * HC)
        def _(i):
            h, Y = i // HC, i % HC
            t = D[h, Y, pl.ds(0, WC, stride=RATIO), :]
            for k in range(1, RATIO):
                t = t + D[h, Y, pl.ds(k, WC, stride=RATIO), :]
            dst[h, DEEP + Y, 16:16 + WC, :] = f(t)

    ysrc = {-1: (DEEP, DEEP), 0: (DEEP, HC), 1: (HC, DEEP)}
    ydst = {-1: (DEEP + HC, DEEP), 0: (DEEP, HC), 1: (0, DEEP)}
    xsrc = {-1: (16, 8), 0: (16, WC), 1: (8 + WC, 8)}
    xdst = {-1: (16 + WC, 8), 0: (16, WC), 1: (8, 8)}

    def send_coarse(buf, k):
        copies = []
        for n, (dy, dx) in enumerate(eight):
            c = pltpu.make_async_remote_copy(
                src_ref=buf.at[:, pl.ds(*ysrc[dy]), pl.ds(*xsrc[dx]), :],
                dst_ref=buf.at[:, pl.ds(*ydst[dy]), pl.ds(*xdst[dx]), :],
                send_sem=cs_sem.at[k, n], recv_sem=cr_sem.at[k, n],
                device_id={"py": ypos[dy], "px": xpos[dx]}, device_id_type=MESH)
            c.start()
            copies.append(c)
        return copies

    def relax_coarse(src, dst, low, high, xlow, xhigh):
        @pl.loop(0, halves)
        def _(h):
            @pl.loop(low, high)
            def _(y):
                for x in range(xlow, xhigh, 8):
                    nb = (src[h, y - 1, x:x + 8, :] + src[h, y + 1, x:x + 8, :]) + (
                        src[h, y, x - 1:x + 7, :] + src[h, y, x + 1:x + 9, :])
                    dst[h, y, x:x + 8, :] = 0.2 * src[h, y, x:x + 8, :] + (
                        CL[h, y, x:x + 8, :] + nb) * CR[h, y, x:x + 8, :]

    for c in u_loads:
        c.wait()
    fine0 = send_fine(U, 0)
    for k in range(CHUNKS):
        for c in chunk_loads[k]:
            c.wait()
        groups = step // RATIO

        @pl.loop(0, halves * groups)
        def _(i):
            h, Y = i // groups, k * groups + i % groups
            for x in range(0, W, 8):
                total = None
                for j in range(RATIO):
                    m = Q[h, RATIO * Y + j, x:x + 8, :]
                    total = m if total is None else total + m
                    q = 4.0 + m
                    Q[h, RATIO * Y + j, x:x + 8, :] = q
                    R[h, RATIO * Y + j, x:x + 8, :] = 0.8 / q
                D[h, Y, x:x + 8, :] = total

    reduce_into(CR, lambda t: 0.8 / (4.0 + 0.25 * t))
    masses = send_coarse(CR, 0)
    for c in s_loads:
        c.wait()
    inner(relax(U, V))
    land_fine(U, 0, fine0)
    rim(relax(U, V))
    fine1 = send_fine(V, 1)
    inner(relax(V, U))
    land_fine(V, 1, fine1)
    rim(relax(V, U))
    fine2 = send_fine(U, 2)
    inner(defect(U))
    land_fine(U, 2, fine2)
    rim(defect(U))

    reduce_into(CL, lambda t: 0.25 * t)
    for c in masses:
        c.wait()
    loads = send_coarse(CL, 1)
    for c in loads:
        c.wait()
    TOP = HC + 2 * DEEP

    @pl.loop(0, halves)
    def _(h):
        @pl.loop(0, TOP)
        def _(y):
            CA[h, y, 8:24 + WC, :] = CL[h, y, 8:24 + WC, :] * CR[h, y, 8:24 + WC, :]

    src, dst = CA, CB
    for n in range(1, DEEP):
        last = n == DEEP - 1
        if last:
            relax_coarse(src, CE, DEEP, DEEP + HC, 16, 16 + WC)
        else:
            relax_coarse(src, dst, n, TOP - n, 8, 24 + WC)
            src, dst = dst, src
    values = send_coarse(CE, 2)
    for c in values:
        c.wait()
    src, dst = CE, CA
    spare = [CA, CB]
    for n in range(1, INNER - DEEP + 1):
        dst = spare[n % 2]
        relax_coarse(src, dst, n, TOP - n, 8, 24 + WC)
        src = dst
    coarse = src

    def add_coarse(h, Yc, rows):
        for k in range(RATIO):
            SP[pl.ds(k, WC + 8, stride=RATIO), :] = coarse[h, Yc, 14:14 + WC + 8, :]
        for row in rows:
            for x in range(0, XW, 8):
                V[h, row, x:x + 8, :] = U[h, row, x:x + 8, :] + SP[x:x + 8, :]

    @pl.loop(0, halves)
    def _(h):
        add_coarse(h, DEEP - 1, [0])
        add_coarse(h, DEEP + HC, [H + 1])

    @pl.loop(0, halves * HC)
    def _(i):
        h, Y = i // HC, i % HC
        add_coarse(h, DEEP + Y, [RATIO * Y + 1 + j for j in range(RATIO)])

    rim(relax(V, U))
    fine3 = send_fine(U, 3)
    inner(relax(V, U))
    inner(relax(U, V))
    land_fine(U, 3, fine3)
    rim(relax(U, V))
    outs = [pltpu.make_async_copy(
        V.at[h, pl.ds(1, H), pl.ds(8, W), :], out_hbm.at[:, :, pl.ds(h * LANES, LANES)],
        out_sem.at[h]) for h in range(halves)]
    for c in outs:
        c.start()
    for c in outs:
        c.wait()


def local(source_terms, initial_values, absorption):
    H, W, cases = source_terms.shape
    halves = cases // LANES
    HC, WC = H // RATIO, W // RATIO
    f32 = jnp.float32
    coarse = pltpu.VMEM((halves, HC + 2 * DEEP, WC + 32, LANES), f32)
    fine = pltpu.VMEM((halves, H + 2, W + 16, LANES), f32)
    plain = pltpu.VMEM((halves, H, W, LANES), f32)
    hbm = pl.BlockSpec(memory_space=pl.ANY)
    return pl.pallas_call(
        functools.partial(kernel, (H, W, halves)),
        out_shape=jax.ShapeDtypeStruct((H, W, cases), f32),
        in_specs=[hbm] * 3,
        out_specs=hbm,
        scratch_shapes=[
            fine, fine, plain, plain, plain,
            pltpu.VMEM((halves, HC, W, LANES), f32),
            coarse, coarse, coarse, coarse, coarse,
            pltpu.VMEM((W + 32, LANES), f32),
            pltpu.VMEM((4, 2, halves, W, LANES), f32),
            pltpu.VMEM((4, 2, halves, H, LANES), f32),
            pltpu.VMEM((4, 2, halves, H, LANES), f32),
            pltpu.SemaphoreType.DMA((3, CHUNKS, halves)),
            pltpu.SemaphoreType.DMA((halves,)),
            pltpu.SemaphoreType.DMA((4, 4)),
            pltpu.SemaphoreType.DMA((4, 4)),
            pltpu.SemaphoreType.DMA((3, 8)),
            pltpu.SemaphoreType.DMA((3, 8)),
        ],
        compiler_params=pltpu.CompilerParams(
            collective_id=0, has_side_effects=True, vmem_limit_bytes=63 * 1024 * 1024),
        name="two_grid",
    )(source_terms, initial_values, absorption)


def solution(mesh):
    return jax.shard_map(
        local,
        mesh=mesh,
        in_specs=(P("py", "px", None), P("py", "px", None), P("py", "px", None)),
        out_specs=P("py", "px", None),
        check_vma=False,
    )
```

```python
import functools

import jax
import jax.numpy as jnp
from jax import lax
from jax.experimental import pallas as pl
from jax.experimental.pallas import tpu as pltpu
from jax.sharding import PartitionSpec as P

RATIO = 4
INNER = 13
LANES = 128
DEEP = 7
MESH = pl.DeviceIdType.MESH
CHUNKS = 4


def kernel(shape, s_hbm, u_hbm, a_hbm, out, U, V, S, R, D, CL, CR, CA, CB, CE, SP,
           RR, RC, PC, in_sem, fs_sem, fr_sem, cs_sem, cr_sem):
    H, W, halves = shape
    HC, WC = H // RATIO, W // RATIO
    XW = W + 16
    npy, npx = lax.axis_size("py"), lax.axis_size("px")
    py, px = lax.axis_index("py"), lax.axis_index("px")
    ypos = {-1: lax.rem(py + npy - 1, npy), 0: py, 1: lax.rem(py + 1, npy)}
    xpos = {-1: lax.rem(px + npx - 1, npx), 0: px, 1: lax.rem(px + 1, npx)}
    eight = [(dy, dx) for dy in (-1, 0, 1) for dx in (-1, 0, 1) if dy or dx]

    def load(hbm, dst, row0, rows, half, sem):
        return pltpu.make_async_copy(
            hbm.at[pl.ds(row0, rows), :, pl.ds(half * LANES, LANES)], dst, sem)

    u_loads = [load(u_hbm, U.at[h, pl.ds(1, H), pl.ds(8, W), :], 0, H, h, in_sem.at[0, 0, h])
               for h in range(halves)]
    for c in u_loads:
        c.start()
    step = H // CHUNKS
    chunk_loads = []
    for k in range(CHUNKS):
        row = []
        rows = pl.ds(k * step, step)
        row.append(pltpu.make_async_copy(a_hbm.at[rows], out.at[rows], in_sem.at[1, k, 0]))
        for c in row:
            c.start()
        chunk_loads.append(row)
    s_loads = [load(s_hbm, S.at[h], 0, H, h, in_sem.at[2, 0, h]) for h in range(halves)]
    for c in s_loads:
        c.start()

    barrier = pltpu.get_barrier_semaphore()
    for dy, dx in eight:
        pl.semaphore_signal(barrier, inc=1, device_id={"py": ypos[dy], "px": xpos[dx]},
                            device_id_type=MESH)
    pl.semaphore_wait(barrier, 8)

    def flat(buf):
        return buf.reshape(halves * (H + 2) * XW, LANES)

    def send_fine(buf, k):
        rows = []
        for n, (dy, row) in enumerate(((-1, 1), (1, H))):
            c = pltpu.make_async_remote_copy(
                src_ref=buf.at[:, row, pl.ds(8, W), :], dst_ref=RR.at[k, n],
                send_sem=fs_sem.at[k, n], recv_sem=fr_sem.at[k, n],
                device_id={"py": ypos[dy], "px": px}, device_id_type=MESH)
            c.start()
            rows.append(c)
        f = flat(buf)
        for n, (dx, col) in enumerate(((-1, 8), (1, 7 + W))):
            for h in range(halves):
                for g in range(0, H, 8):
                    PC[k, n, h, g:g + 8, :] = f[
                        pl.ds((h * (H + 2) + 1 + g) * XW + col, 8, stride=XW), :]
            c = pltpu.make_async_remote_copy(
                src_ref=PC.at[k, n], dst_ref=RC.at[k, n],
                send_sem=fs_sem.at[k, 2 + n], recv_sem=fr_sem.at[k, 2 + n],
                device_id={"py": py, "px": xpos[dx]}, device_id_type=MESH)
            c.start()
            rows.append(c)
        return rows

    def land_fine(buf, k, copies):
        for c in copies:
            c.wait()
        for n, row in enumerate((H + 1, 0)):
            for h in range(halves):
                buf[h, row, 8:8 + W, :] = RR[k, n, h]
        f = flat(buf)
        for n, col in enumerate((8 + W, 7)):
            for h in range(halves):
                for g in range(0, H, 8):
                    f[pl.ds((h * (H + 2) + 1 + g) * XW + col, 8, stride=XW), :] = (
                        RC[k, n, h, g:g + 8, :])

    def lanes(h):
        return pl.ds(pl.multiple_of(h * LANES, LANES), LANES)

    def around(buf, h, Y, x):
        base = RATIO * Y
        c = [buf[h, base + i, x:x + 8, :] for i in range(RATIO + 2)]
        for i in range(RATIO):
            left = buf[h, base + 1 + i, x - 1:x + 7, :]
            right = buf[h, base + 1 + i, x + 1:x + 9, :]
            yield base + i, c[i + 1], (c[i] + c[i + 2]) + (left + right)

    def relax(src, dst=None):
        def unit(h, Y, x):
            for y, mid, nb in around(src, h, Y, x):
                new = 0.2 * mid + (S[h, y, x - 8:x, :] + nb) * R[h, y, x - 8:x, :]
                if dst is None:
                    out[y, x - 8:x, lanes(h)] = new
                else:
                    dst[h, y + 1, x:x + 8, :] = new
        return unit

    def defect(src):
        def unit(h, Y, x):
            total = None
            for y, mid, nb in around(src, h, Y, x):
                d = (S[h, y, x - 8:x, :] + nb) - out[y, x - 8:x, lanes(h)] * mid
                total = d if total is None else total + d
            D[h, Y, x - 8:x, :] = total
        return unit

    def inner(unit):
        @pl.loop(0, halves * (HC - 2))
        def _(i):
            h, Y = i // (HC - 2), 1 + i % (HC - 2)
            for x in range(16, W, 8):
                unit(h, Y, x)

    def rim(unit):
        @pl.loop(0, halves * 2)
        def _(i):
            h, Y = i // 2, (i % 2) * (HC - 1)
            for x in range(8, W + 8, 8):
                unit(h, Y, x)

        @pl.loop(0, halves * (HC - 2))
        def _(i):
            h, Y = i // (HC - 2), 1 + i % (HC - 2)
            unit(h, Y, 8)
            unit(h, Y, W)

    def reduce_into(dst, f):
        @pl.loop(0, halves * HC)
        def _(i):
            h, Y = i // HC, i % HC
            t = D[h, Y, pl.ds(0, WC, stride=RATIO), :]
            for k in range(1, RATIO):
                t = t + D[h, Y, pl.ds(k, WC, stride=RATIO), :]
            dst[h, DEEP + Y, 16:16 + WC, :] = f(t)

    ysrc = {-1: (DEEP, DEEP), 0: (DEEP, HC), 1: (HC, DEEP)}
    ydst = {-1: (DEEP + HC, DEEP), 0: (DEEP, HC), 1: (0, DEEP)}
    xsrc = {-1: (16, 8), 0: (16, WC), 1: (8 + WC, 8)}
    xdst = {-1: (16 + WC, 8), 0: (16, WC), 1: (8, 8)}

    def send_coarse(buf, k):
        copies = []
        for n, (dy, dx) in enumerate(eight):
            c = pltpu.make_async_remote_copy(
                src_ref=buf.at[:, pl.ds(*ysrc[dy]), pl.ds(*xsrc[dx]), :],
                dst_ref=buf.at[:, pl.ds(*ydst[dy]), pl.ds(*xdst[dx]), :],
                send_sem=cs_sem.at[k, n], recv_sem=cr_sem.at[k, n],
                device_id={"py": ypos[dy], "px": xpos[dx]}, device_id_type=MESH)
            c.start()
            copies.append(c)
        return copies

    def relax_coarse(src, dst, low, high, xlow, xhigh):
        @pl.loop(0, (high - low) // 2)
        def _(i):
            y = low + 2 * i
            for h in range(halves):
                for x in range(xlow, xhigh, 8):
                    c = [src[h, y - 1 + j, x:x + 8, :] for j in range(4)]
                    for j in range(2):
                        nb = (c[j] + c[j + 2]) + (
                            src[h, y + j, x - 1:x + 7, :] + src[h, y + j, x + 1:x + 9, :])
                        dst[h, y + j, x:x + 8, :] = 0.2 * c[j + 1] + (
                            CL[h, y + j, x:x + 8, :] + nb) * CR[h, y + j, x:x + 8, :]

    for c in u_loads:
        c.wait()
    fine0 = send_fine(U, 0)
    for k in range(CHUNKS):
        for c in chunk_loads[k]:
            c.wait()
        groups = step // RATIO

        @pl.loop(0, halves * groups)
        def _(i):
            h, Y = i // groups, k * groups + i % groups
            for x in range(0, W, 8):
                total = None
                for j in range(RATIO):
                    m = out[RATIO * Y + j, x:x + 8, lanes(h)]
                    total = m if total is None else total + m
                    q = 4.0 + m
                    out[RATIO * Y + j, x:x + 8, lanes(h)] = q
                    R[h, RATIO * Y + j, x:x + 8, :] = 0.8 / q
                D[h, Y, x:x + 8, :] = total

    reduce_into(CR, lambda t: 0.8 / (4.0 + 0.25 * t))
    masses = send_coarse(CR, 0)
    for c in s_loads:
        c.wait()
    inner(relax(U, V))
    land_fine(U, 0, fine0)
    rim(relax(U, V))
    fine1 = send_fine(V, 1)
    inner(relax(V, U))
    land_fine(V, 1, fine1)
    rim(relax(V, U))
    fine2 = send_fine(U, 2)
    inner(defect(U))
    land_fine(U, 2, fine2)
    rim(defect(U))

    reduce_into(CL, lambda t: 0.25 * t)
    for c in masses:
        c.wait()
    loads = send_coarse(CL, 1)
    for c in loads:
        c.wait()
    TOP = HC + 2 * DEEP

    @pl.loop(0, halves)
    def _(h):
        @pl.loop(0, TOP)
        def _(y):
            CA[h, y, 8:24 + WC, :] = CL[h, y, 8:24 + WC, :] * CR[h, y, 8:24 + WC, :]

    src, dst = CA, CB
    for n in range(1, DEEP):
        last = n == DEEP - 1
        if last:
            relax_coarse(src, CE, DEEP, DEEP + HC, 16, 16 + WC)
        else:
            relax_coarse(src, dst, n, TOP - n, 8, 24 + WC)
            src, dst = dst, src
    values = send_coarse(CE, 2)
    for c in values:
        c.wait()
    src, dst = CE, CA
    spare = [CA, CB]
    for n in range(1, INNER - DEEP + 1):
        dst = spare[n % 2]
        relax_coarse(src, dst, n, TOP - n, 8, 24 + WC)
        src = dst
    coarse = src

    def add_coarse(h, Yc, rows):
        for k in range(RATIO):
            SP[pl.ds(k, WC + 8, stride=RATIO), :] = coarse[h, Yc, 14:14 + WC + 8, :]
        for row in rows:
            for x in range(0, XW, 8):
                V[h, row, x:x + 8, :] = U[h, row, x:x + 8, :] + SP[x:x + 8, :]

    @pl.loop(0, halves)
    def _(h):
        add_coarse(h, DEEP - 1, [0])
        add_coarse(h, DEEP + HC, [H + 1])

    @pl.loop(0, halves * HC)
    def _(i):
        h, Y = i // HC, i % HC
        add_coarse(h, DEEP + Y, [RATIO * Y + 1 + j for j in range(RATIO)])

    rim(relax(V, U))
    fine3 = send_fine(U, 3)
    inner(relax(V, U))
    inner(relax(U))
    land_fine(U, 3, fine3)
    rim(relax(U))


def local(source_terms, initial_values, absorption):
    H, W, cases = source_terms.shape
    halves = cases // LANES
    HC, WC = H // RATIO, W // RATIO
    f32 = jnp.float32
    coarse = pltpu.VMEM((halves, HC + 2 * DEEP, WC + 32, LANES), f32)
    fine = pltpu.VMEM((halves, H + 2, W + 16, LANES), f32)
    plain = pltpu.VMEM((halves, H, W, LANES), f32)
    hbm = pl.BlockSpec(memory_space=pl.ANY)
    return pl.pallas_call(
        functools.partial(kernel, (H, W, halves)),
        out_shape=pltpu.VMEM((H, W, cases), f32),
        in_specs=[hbm] * 3,
        out_specs=pl.BlockSpec(memory_space=pltpu.VMEM),
        scratch_shapes=[
            fine, fine, plain, plain,
            pltpu.VMEM((halves, HC, W, LANES), f32),
            coarse, coarse, coarse, coarse, coarse,
            pltpu.VMEM((W + 32, LANES), f32),
            pltpu.VMEM((4, 2, halves, W, LANES), f32),
            pltpu.VMEM((4, 2, halves, H, LANES), f32),
            pltpu.VMEM((4, 2, halves, H, LANES), f32),
            pltpu.SemaphoreType.DMA((3, CHUNKS, halves)),
            pltpu.SemaphoreType.DMA((4, 4)),
            pltpu.SemaphoreType.DMA((4, 4)),
            pltpu.SemaphoreType.DMA((3, 8)),
            pltpu.SemaphoreType.DMA((3, 8)),
        ],
        compiler_params=pltpu.CompilerParams(
            collective_id=0, has_side_effects=True, vmem_limit_bytes=52 * 1024 * 1024),
        name="two_grid",
    )(source_terms, initial_values, absorption)


def solution(mesh):
    return jax.shard_map(
        local,
        mesh=mesh,
        in_specs=(P("py", "px", None), P("py", "px", None), P("py", "px", None)),
        out_specs=P("py", "px", None),
        check_vma=False,
    )
```
